32 devices in a mesh: level: 4 (over x, core), space: 8 (over z, y).
Axes of the slice: x: 2, y: 2, z: 4, core: 2. Of those that a mesh axis runs over, the one named last changes fastest.
Arguments:
- u_init: float32 [256, 2048], P('space'), may hold values from 0.2 to 1
- v_init: float32 [256, 2048], P('space'), may hold values from 0 to 0.5
- feed_rate: float32 [256, 2048], P('space'), may hold values from 0.01 to 0.12
- kill_rate: float32 [256, 2048], P('space'), may hold values from 0.02 to 0.16
Outputs:
- level_states: float32 [4, 2, 256, 2048], P('level', None, 'space')
The draws below stay inside these ranges and needn't reach their ends.
All inputs are finite; a program needn't handle non-finite values.
Results may differ from the reference program's by a relative error of at most 0.0003.
Values sent between devices are 32-bit elements; how exact they have to be, the bound alone decides.
A program may use at most 64 MiB of HBM per device.

```python
import math
import jax
import jax.numpy as jnp
from jax import lax

NX = 2048
STEPS = 4
SWEEPS = 3
NY = 256
N_LEVEL = 4


def block_levels(stream_key, shape, cuts, least, top_value):
    gain = 1.0
    for axis_at, shards_of in cuts:
        draws = jax.random.uniform(jax.random.fold_in(jax.random.fold_in(stream_key, 6), axis_at), (shards_of,), jnp.float32, least / len(cuts), top_value / len(cuts))
        gain = gain * jnp.repeat(jnp.exp(draws), shape[axis_at] // shards_of).reshape((-1,) + (1,) * (len(shape) - 1 - axis_at))
    return gain


def setup_inputs(seed: int = 0) -> dict:
    splits = jax.random.split(jax.random.key(seed), 5)
    return {
        "u_init": jnp.clip(0.2 + 0.8 * jax.random.uniform(splits[0], (NY, NX), jnp.float32) ** block_levels(splits[0], (NY, NX), ((0, 8),), -0.2, 0.2), 0.2, 1.0),
        "v_init": jnp.clip(0.5 * jax.random.uniform(splits[1], (NY, NX), jnp.float32) ** block_levels(splits[1], (NY, NX), ((0, 8),), -0.2, 0.2), 0.0, 0.5),
        "feed_rate": jnp.clip(jnp.exp(math.log(0.12) - 2.4849066 * jax.random.uniform(splits[2], (NY, NX), jnp.float32) ** block_levels(splits[2], (NY, NX), ((0, 8),), -0.2, 0.2)), 0.01, 0.12),
        "kill_rate": jnp.clip(jnp.exp(math.log(0.16) - 2.0794415 * jax.random.uniform(splits[3], (NY, NX), jnp.float32) ** block_levels(splits[3], (NY, NX), ((0, 8),), -0.2, 0.2)), 0.02, 0.16),
    }


time_step = 1.0
diffusion = (1.0, 0.5)
quad_weights = [[9.0, 19.0, -5.0, 1.0, 0.0], [-1.0, 13.0, 13.0, -1.0, 0.0], [1.0, -5.0, 19.0, 9.0, 0.0], [0.0, 1.0, -5.0, 19.0, 9.0]]


def diffusion_rates():
    return jnp.array(diffusion, jnp.float32)[:, None, None]


def reaction(state, feed_rate, kill_rate):
    u_field = state[0]
    v_field = state[1]
    uv_square = u_field * v_field * v_field
    return jnp.stack([-uv_square + feed_rate * (1.0 - u_field), uv_square - (feed_rate + kill_rate) * v_field])


def neighbours(iterate):
    return jnp.roll(iterate, 1, 1) + jnp.roll(iterate, -1, 1) + jnp.roll(iterate, 1, 2) + jnp.roll(iterate, -1, 2)


def laplace(state):
    return diffusion_rates() * (neighbours(state) - 4.0 * state)


def jacobi_solve(source):
    step_rate = time_step * diffusion_rates()
    iterate = source
    for sweep_idx in range(SWEEPS):
        iterate = (source + step_rate * neighbours(iterate)) / (1.0 + 4.0 * step_rate)
    return iterate


def reference(u_init, v_init, feed_rate, kill_rate):
    weight_table = jnp.array(quad_weights, jnp.float32) / 24.0
    initial = jnp.stack([u_init, v_init])
    prev_lap = None
    prev_rea = None
    final_list = []
    for level_idx in range(N_LEVEL):
        state = initial
        node_list = [initial]
        for step_idx in range(STEPS):
            source = state + time_step * reaction(state, feed_rate, kill_rate)
            if level_idx > 0:
                forcing = prev_lap + prev_rea
                quadrature = time_step * jnp.einsum("m,mfij->fij", weight_table[step_idx], forcing, precision=lax.Precision.HIGHEST)
                source = source + (quadrature - time_step * prev_lap[step_idx + 1] - time_step * prev_rea[step_idx])
            state = jacobi_solve(source)
            node_list.append(state)
        final_list.append(state)
        prev_lap = jnp.stack([laplace(node_value) for node_value in node_list])
        prev_rea = jnp.stack([reaction(node_value, feed_rate, kill_rate) for node_value in node_list])
    return jnp.stack(final_list)
```

```python
import functools

import jax
import jax.numpy as jnp
from jax import lax
from jax.experimental import pallas as pl
from jax.experimental.pallas import tpu as pltpu
from jax.sharding import PartitionSpec as P

STEPS = 4
SWEEPS = 3
LANES = 128
SUB = 8
HALF = LANES // 2
FAR = 16
CHUNK = 3

DIFF = (1.0, 0.5)
INV = tuple(1.0 / (1.0 + 4.0 * d) for d in DIFF)
GAIN = tuple(d / (1.0 + 4.0 * d) for d in DIFF)
W = [
    [9.0, 19.0, -5.0, 1.0, 0.0],
    [-1.0, 13.0, 13.0, -1.0, 0.0],
    [1.0, -5.0, 19.0, 9.0, 0.0],
    [0.0, 1.0, -5.0, 19.0, 9.0],
]
MESH = pl.DeviceIdType.MESH


def kernel(
    levels, spaces, tiles, start, u_ref, v_ref, f_ref, k_ref, out_ref,
    send, grid_in, feed, drain, y, lap, rea, corr, rhs, za, zb, nat, pack, recv,
    g_send, g_recv, o_send, o_recv, loc_sem,
):
    lev = lax.axis_index("level")
    spc = lax.axis_index("space")
    rows, width = u_ref.shape
    all_tiles = width // LANES
    pairs = spaces // 2
    pair, side = spc // 2, lax.rem(spc, 2)
    block_tiles = all_tiles // (2 * levels)
    win = block_tiles + 1
    nxt = lax.rem(pair + 1, pairs)
    prv = lax.rem(pair + pairs - 1, pairs)
    block = 2 * lev + side
    own_lo = FAR + rows

    for q, ref in enumerate((u_ref, v_ref, f_ref, k_ref)):
        for j in range(all_tiles + 1):
            jj = j % all_tiles
            send[j, q] = ref[:, jj * LANES : (jj + 1) * LANES]

    barrier = pltpu.get_barrier_semaphore()
    count = 0
    for p in (nxt, prv):
        for s in range(2):
            pl.semaphore_signal(barrier, inc=1, device_id=(lev, 2 * p + s), device_id_type=MESH)
            count += 1
    for dl in range(levels):
        for ds in range(2):
            if dl == 0 and ds == 0:
                continue
            pl.semaphore_signal(
                barrier, inc=1,
                device_id=(lax.rem(lev + dl, levels), 2 * pair + lax.rem(side + ds, 2)),
                device_id_type=MESH,
            )
            count += 1
    pl.semaphore_wait(barrier, count)

    def remote(win_side, r0, n, d0, sem, target, slot):
        return pltpu.make_async_remote_copy(
            src_ref=send.at[pl.ds(block_tiles * (2 * lev + win_side), win), :, pl.ds(r0, n), :],
            dst_ref=grid_in.at[:, :, pl.ds(d0, n), :],
            send_sem=g_send.at[slot], recv_sem=g_recv.at[sem],
            device_id=(lev, target), device_id_type=MESH,
        )

    def gather_copies(s):
        copies = [remote(1 - s, 0, rows, own_lo + rows * s, 0, 2 * pair + 1 - s, 0)]
        for i, t in enumerate((s, 1 - s)):
            if s == 0:
                copies.append(remote(t, rows - FAR, FAR, 0, 1, 2 * nxt + t, 1 + i))
                copies.append(remote(t, 0, rows, own_lo + 2 * rows, 3, 2 * prv + t, 3 + i))
            else:
                copies.append(remote(t, 0, rows, FAR, 2, 2 * nxt + t, 1 + i))
                copies.append(remote(t, 0, FAR, own_lo + 3 * rows, 4, 2 * prv + t, 3 + i))
        return copies

    for s in range(2):
        @pl.when(side == s)
        def _(s=s):
            for c in gather_copies(s):
                c.start()
    own = pltpu.make_async_copy(
        send.at[pl.ds(block_tiles * block, win)],
        grid_in.at[:, :, pl.ds(pl.multiple_of(own_lo + rows * side, SUB), rows), :],
        loc_sem.at[0],
    )
    own.start()
    own.wait()
    for sem, n, d0 in (
        (1, FAR, 0), (2, rows, FAR), (3, rows, own_lo + 2 * rows), (4, FAR, own_lo + 3 * rows)
    ):
        remote(0, 0, n, d0, sem, 2 * nxt, 0).wait_recv()
    remote(0, 0, rows, pl.multiple_of(own_lo + rows * (1 - side), SUB), 0, 2 * nxt, 0).wait_recv()
    for s in range(2):
        @pl.when(side == s)
        def _(s=s):
            for c in gather_copies(s):
                c.wait_send()

    chunks = [(a, min(a + CHUNK, tiles)) for a in range(0, tiles, CHUNK)]
    wide = win * LANES

    def put(ref, q, a, b, val):
        ref[q, a + 1 : b + 1] = val
        if a == 0:
            ref[q, tiles + 1] = pltpu.roll(val[0], SUB - 1, 0)
        if b == tiles:
            ref[q, 0] = pltpu.roll(val[b - a - 1], 1, 0)

    def around(ref, q, a, b):
        mid = ref[q, a + 1 : b + 1]
        flat = mid.reshape((b - a) * SUB, wide)
        cols = pltpu.roll(flat, 1, 1) + pltpu.roll(flat, wide - 1, 1)
        return (ref[q, a:b] + ref[q, a + 2 : b + 2]) + cols.reshape(b - a, SUB, wide), mid

    def rates(node):
        for a, b in chunks:
            nu, u = around(y.at[node], 0, a, b)
            nv, v = around(y.at[node], 1, a, b)
            lap[node, 0, a:b] = DIFF[0] * (nu - 4.0 * u)
            lap[node, 1, a:b] = DIFF[1] * (nv - 4.0 * v)
            uvv = u * v * v
            rea[node, 0, a:b] = feed[a:b] * (1.0 - u) - uvv
            rea[node, 1, a:b] = uvv - drain[a:b] * v

    for t in range(tiles):
        def window(q, t=t):
            return jnp.concatenate(
                [grid_in[j, q, pl.ds(start + t, SUB, stride=tiles), :] for j in range(win)], axis=1
            )
        fd = window(2)
        feed[t] = fd
        drain[t] = fd + window(3)
        for q in range(2):
            put(y.at[0], q, t, t + 1, window(q)[None])
    rates(0)

    def section(n, corrected):
        for q in range(2):
            for a, b in chunks:
                src = y[n, q, a + 1 : b + 1] + rea[n, q, a:b]
                if corrected:
                    src = src + corr[n, q, a:b]
                put(rhs, q, a, b, src * INV[q])
        for old, new, coef in ((rhs, za, DIFF), (za, zb, GAIN), (zb, y.at[n + 1], GAIN)):
            for q in range(2):
                for a, b in chunks:
                    total, _ = around(old, q, a, b)
                    put(new, q, a, b, rhs[q, a + 1 : b + 1] + coef[q] * total)
        rates(n + 1)

    def out_copy(level, s):
        return pltpu.make_async_remote_copy(
            src_ref=pack.at[level, s], dst_ref=recv.at[block],
            send_sem=o_send.at[level, s], recv_sem=o_recv.at[block],
            device_id=(level, 2 * pair + s), device_id_type=MESH,
        )

    low = lax.broadcasted_iota(jnp.int32, (2 * rows, LANES), 1) < HALF

    def emit(level):
        for q in range(2):
            for t in range(tiles):
                row = y[STEPS, q, t + 1]
                for j in range(win):
                    nat[j, q, pl.ds(start + t, SUB, stride=tiles), :] = row[:, j * LANES : (j + 1) * LANES]
            for j in range(block_tiles):
                val = nat[j, q, own_lo : own_lo + 2 * rows]
                if j == 0:
                    val = jnp.where(low, nat[block_tiles, q, own_lo : own_lo + 2 * rows], val)
                for s in range(2):
                    pack[level, s, j, q] = val[s * rows : (s + 1) * rows]
        for s in range(2):
            mine = (level == lev) & (side == s)

            @pl.when(mine)
            def _(s=s):
                pltpu.make_async_copy(pack.at[level, s], recv.at[block], loc_sem.at[1]).start()

            @pl.when(jnp.logical_not(mine))
            def _(s=s):
                out_copy(level, s).start()

    def step0(n, c):
        section(n, False)
        return c

    lax.fori_loop(0, STEPS, step0, 0)
    emit(0)

    def one_level(level, c):
        def correction(t, c):
            for q in range(2):
                laps = [lap[m, q, t] for m in range(STEPS + 1)]
                reas = [rea[m, q, t] for m in range(STEPS + 1)]
                both = [a + b for a, b in zip(laps, reas)]
                for n in range(STEPS):
                    acc = None
                    for m in range(STEPS + 1):
                        if W[n][m] != 0.0:
                            term = (W[n][m] / 24.0) * both[m]
                            acc = term if acc is None else acc + term
                    corr[n, q, t] = acc - laps[n + 1] - reas[n]
            return c

        lax.fori_loop(0, tiles, correction, 0)

        def step(n, c):
            section(n, True)
            return c

        lax.fori_loop(0, STEPS, step, 0)
        emit(level)
        return c

    lax.fori_loop(1, levels, one_level, 0)

    for level in range(levels):
        for s in range(2):
            mine = (lev == level) & (side == s)

            @pl.when(mine)
            def _(level=level, s=s):
                pltpu.make_async_copy(pack.at[level, s], recv.at[block], loc_sem.at[1]).wait()

            @pl.when(jnp.logical_not(mine))
            def _(level=level, s=s):
                out_copy(level, s).wait_send()
    for b in range(2 * levels):
        @pl.when(block != b)
        def _(b=b):
            pltpu.make_async_remote_copy(
                src_ref=pack.at[0, 0], dst_ref=recv.at[b],
                send_sem=o_send.at[0, 0], recv_sem=o_recv.at[b],
                device_id=(lev, 2 * pair + 1 - side), device_id_type=MESH,
            ).wait_recv()
    low1 = lax.broadcasted_iota(jnp.int32, (rows, LANES), 1) < HALF
    for b in range(2 * levels):
        before = (b + 2 * levels - 1) % (2 * levels)
        for q in range(2):
            for j in range(block_tiles):
                val = recv[b, j, q]
                if j == 0:
                    val = jnp.where(low1, recv[before, 0, q], val)
                at = (b * block_tiles + j) * LANES
                out_ref[0, q, :, at : at + LANES] = val


def body(u_init, v_init, feed_rate, kill_rate):
    rows, width = u_init.shape
    levels = lax.axis_size("level")
    spaces = lax.axis_size("space")
    block_tiles = width // LANES // (2 * levels)
    win = block_tiles + 1
    wide = win * LANES
    tall = 4 * rows + 2 * FAR
    need = STEPS * SWEEPS + (levels - 1) * (SWEEPS * (STEPS - 1) + 1)
    tiles = -(-(2 * rows + 2 * need) // SUB)
    start = (tall - tiles * SUB) // 2
    assert start >= 0 and need <= HALF
    f32 = jnp.float32
    ghost = (2, tiles + 2, SUB, wide)
    plain = (2, tiles, SUB, wide)
    scratch = [
        pltpu.VMEM((width // LANES + 1, 4, rows, LANES), f32),
        pltpu.VMEM((win, 4, tall, LANES), f32),
        pltpu.VMEM(plain[1:], f32),
        pltpu.VMEM(plain[1:], f32),
        pltpu.VMEM((STEPS + 1,) + ghost, f32),
        pltpu.VMEM((STEPS + 1,) + plain, f32),
        pltpu.VMEM((STEPS + 1,) + plain, f32),
        pltpu.VMEM((STEPS,) + plain, f32),
        pltpu.VMEM(ghost, f32),
        pltpu.VMEM(ghost, f32),
        pltpu.VMEM(ghost, f32),
        pltpu.VMEM((win, 2, tall, LANES), f32),
        pltpu.VMEM((levels, 2, block_tiles, 2, rows, LANES), f32),
        pltpu.VMEM((2 * levels, block_tiles, 2, rows, LANES), f32),
        pltpu.SemaphoreType.DMA((5,)),
        pltpu.SemaphoreType.DMA((5,)),
        pltpu.SemaphoreType.DMA((levels, 2)),
        pltpu.SemaphoreType.DMA((2 * levels,)),
        pltpu.SemaphoreType.DMA((2,)),
    ]
    return pl.pallas_call(
        functools.partial(kernel, levels, spaces, tiles, start),
        out_shape=jax.ShapeDtypeStruct((1, 2, rows, width), f32),
        in_specs=[pl.BlockSpec(memory_space=pltpu.VMEM)] * 4,
        out_specs=pl.BlockSpec(memory_space=pltpu.VMEM),
        scratch_shapes=scratch,
        compiler_params=pltpu.CompilerParams(
            collective_id=0, has_side_effects=True, vmem_limit_bytes=56 * 1024 * 1024
        ),
    )(u_init, v_init, feed_rate, kill_rate)


def solution(mesh):
    return jax.shard_map(
        body,
        mesh=mesh,
        in_specs=(P("space", None),) * 4,
        out_specs=P("level", None, "space", None),
        check_vma=False,
    )
```

```python
import functools

import jax
import jax.numpy as jnp
from jax import lax
from jax.experimental import pallas as pl
from jax.experimental.pallas import tpu as pltpu
from jax.sharding import PartitionSpec as P

STEPS = 4
SWEEPS = 3
LANES = 128
SUB = 8
HALF = LANES // 2
FAR = 16
CHUNK = 3

DIFF = (1.0, 0.5)
INV = tuple(1.0 / (1.0 + 4.0 * d) for d in DIFF)
GAIN = tuple(d / (1.0 + 4.0 * d) for d in DIFF)
W = [
    [9.0, 19.0, -5.0, 1.0, 0.0],
    [-1.0, 13.0, 13.0, -1.0, 0.0],
    [1.0, -5.0, 19.0, 9.0, 0.0],
    [0.0, 1.0, -5.0, 19.0, 9.0],
]
MESH = pl.DeviceIdType.MESH


def kernel(
    levels, spaces, level_tiles, tall, u_ref, v_ref, f_ref, k_ref, out_ref,
    send, grid_in, feed, drain, y, lap, rea, corr, rhs, za, zb, nat, cnat, pack, recv,
    g_send, g_recv, o_send, o_recv, loc_sem,
):
    lev = lax.axis_index("level")
    spc = lax.axis_index("space")
    rows, width = u_ref.shape
    all_tiles = width // LANES
    pairs = spaces // 2
    pair, side = spc // 2, lax.rem(spc, 2)
    block_tiles = all_tiles // (2 * levels)
    win = block_tiles + 1
    nxt = lax.rem(pair + 1, pairs)
    prv = lax.rem(pair + pairs - 1, pairs)
    block = 2 * lev + side
    own_lo = FAR + rows

    for q, ref in enumerate((u_ref, v_ref, f_ref, k_ref)):
        for j in range(all_tiles + 1):
            jj = j % all_tiles
            send[j, q] = ref[:, jj * LANES : (jj + 1) * LANES]

    barrier = pltpu.get_barrier_semaphore()
    count = 0
    for p in (nxt, prv):
        for s in range(2):
            pl.semaphore_signal(barrier, inc=1, device_id=(lev, 2 * p + s), device_id_type=MESH)
            count += 1
    for dl in range(levels):
        for ds in range(2):
            if dl == 0 and ds == 0:
                continue
            pl.semaphore_signal(
                barrier, inc=1,
                device_id=(lax.rem(lev + dl, levels), 2 * pair + lax.rem(side + ds, 2)),
                device_id_type=MESH,
            )
            count += 1
    pl.semaphore_wait(barrier, count)

    def remote(win_side, r0, n, d0, sem, target, slot):
        return pltpu.make_async_remote_copy(
            src_ref=send.at[pl.ds(block_tiles * (2 * lev + win_side), win), :, pl.ds(r0, n), :],
            dst_ref=grid_in.at[:, :, pl.ds(d0, n), :],
            send_sem=g_send.at[slot], recv_sem=g_recv.at[sem],
            device_id=(lev, target), device_id_type=MESH,
        )

    def gather_copies(s):
        copies = [remote(1 - s, 0, rows, own_lo + rows * s, 0, 2 * pair + 1 - s, 0)]
        for i, t in enumerate((s, 1 - s)):
            if s == 0:
                copies.append(remote(t, rows - FAR, FAR, 0, 1, 2 * nxt + t, 1 + i))
                copies.append(remote(t, 0, rows, own_lo + 2 * rows, 3, 2 * prv + t, 3 + i))
            else:
                copies.append(remote(t, 0, rows, FAR, 2, 2 * nxt + t, 1 + i))
                copies.append(remote(t, 0, FAR, own_lo + 3 * rows, 4, 2 * prv + t, 3 + i))
        return copies

    for s in range(2):
        @pl.when(side == s)
        def _(s=s):
            for c in gather_copies(s):
                c.start()
    own = pltpu.make_async_copy(
        send.at[pl.ds(block_tiles * block, win)],
        grid_in.at[:, :, pl.ds(pl.multiple_of(own_lo + rows * side, SUB), rows), :],
        loc_sem.at[0],
    )
    own.start()
    own.wait()
    for sem, n, d0 in (
        (1, FAR, 0), (2, rows, FAR), (3, rows, own_lo + 2 * rows), (4, FAR, own_lo + 3 * rows)
    ):
        remote(0, 0, n, d0, sem, 2 * nxt, 0).wait_recv()
    remote(0, 0, rows, pl.multiple_of(own_lo + rows * (1 - side), SUB), 0, 2 * nxt, 0).wait_recv()
    for s in range(2):
        @pl.when(side == s)
        def _(s=s):
            for c in gather_copies(s):
                c.wait_send()

    wide = win * LANES

    def put(tiles, ref, q, a, b, val):
        ref[q, a + 1 : b + 1] = val
        if a == 0:
            ref[q, tiles + 1] = pltpu.roll(val[0], SUB - 1, 0)
        if b == tiles:
            ref[q, 0] = pltpu.roll(val[b - a - 1], 1, 0)

    def around(ref, q, a, b):
        mid = ref[q, a + 1 : b + 1]
        flat = mid.reshape((b - a) * SUB, wide)
        cols = pltpu.roll(flat, 1, 1) + pltpu.roll(flat, wide - 1, 1)
        return (ref[q, a:b] + ref[q, a + 2 : b + 2]) + cols.reshape(b - a, SUB, wide), mid

    def rates(tiles, node, last=False):
        for a, b in chunks_of(tiles):
            nu, u = around(y.at[node], 0, a, b)
            nv, v = around(y.at[node], 1, a, b)
            if not last:
                lap[node, 0, a:b] = DIFF[0] * (nu - 4.0 * u)
                lap[node, 1, a:b] = DIFF[1] * (nv - 4.0 * v)
            uvv = u * v * v
            rea[node, 0, a:b] = feed[a:b] * (1.0 - u) - uvv
            rea[node, 1, a:b] = uvv - drain[a:b] * v

    def setup(tiles, corrected, last):
        start = (tall - tiles * SUB) // 2
        for t in range(tiles):
            def window(ref, t=t):
                return jnp.concatenate(
                    [ref(j)[pl.ds(start + t, SUB, stride=tiles), :] for j in range(win)], axis=1
                )
            fd = window(lambda j: grid_in.at[j, 2])
            feed[t] = fd
            drain[t] = fd + window(lambda j: grid_in.at[j, 3])
            for q in range(2):
                put(tiles, y.at[0], q, t, t + 1, window(lambda j, q=q: grid_in.at[j, q])[None])
                if corrected:
                    for n in range(STEPS):
                        corr[n, q, t] = window(lambda j, q=q, n=n: cnat.at[n, q, j])
        rates(tiles, 0, last)

    def chunks_of(tiles):
        return [(a, min(a + CHUNK, tiles)) for a in range(0, tiles, CHUNK)]

    def section(tiles, n, corrected, last):
        for q in range(2):
            for a, b in chunks_of(tiles):
                src = y[n, q, a + 1 : b + 1] + rea[n, q, a:b]
                if corrected:
                    src = src + corr[n, q, a:b]
                put(tiles, rhs, q, a, b, src * INV[q])
        for old, new, coef in ((rhs, za, DIFF), (za, zb, GAIN), (zb, y.at[n + 1], GAIN)):
            for q in range(2):
                for a, b in chunks_of(tiles):
                    total, _ = around(old, q, a, b)
                    put(tiles, new, q, a, b, rhs[q, a + 1 : b + 1] + coef[q] * total)
        rates(tiles, n + 1, last)

    def out_copy(level, s):
        return pltpu.make_async_remote_copy(
            src_ref=pack.at[level, s], dst_ref=recv.at[block],
            send_sem=o_send.at[level, s], recv_sem=o_recv.at[block],
            device_id=(level, 2 * pair + s), device_id_type=MESH,
        )

    low = lax.broadcasted_iota(jnp.int32, (2 * rows, LANES), 1) < HALF

    def emit(tiles, level):
        start = (tall - tiles * SUB) // 2
        for q in range(2):
            for t in range(tiles):
                row = y[STEPS, q, t + 1]
                for j in range(win):
                    nat[j, q, pl.ds(start + t, SUB, stride=tiles), :] = row[:, j * LANES : (j + 1) * LANES]
            for j in range(block_tiles):
                val = nat[j, q, own_lo : own_lo + 2 * rows]
                if j == 0:
                    val = jnp.where(low, nat[block_tiles, q, own_lo : own_lo + 2 * rows], val)
                for s in range(2):
                    pack[level, s, j, q] = val[s * rows : (s + 1) * rows]
        for s in range(2):
            mine = (level == lev) & (side == s)

            @pl.when(mine)
            def _(s=s):
                pltpu.make_async_copy(pack.at[level, s], recv.at[block], loc_sem.at[1]).start()

            @pl.when(jnp.logical_not(mine))
            def _(s=s):
                out_copy(level, s).start()

    def correct(tiles):
        start = (tall - tiles * SUB) // 2
        for t in range(tiles):
            for q in range(2):
                laps = [lap[m, q, t] for m in range(STEPS + 1)]
                reas = [rea[m, q, t] for m in range(STEPS + 1)]
                both = [a + b for a, b in zip(laps, reas)]
                for n in range(STEPS):
                    acc = -laps[n + 1] - reas[n]
                    for m in range(STEPS + 1):
                        if W[n][m] != 0.0:
                            acc = acc + (W[n][m] / 24.0) * both[m]
                    for j in range(win):
                        cnat[n, q, j, pl.ds(start + t, SUB, stride=tiles), :] = acc[
                            :, j * LANES : (j + 1) * LANES
                        ]

    for level in range(levels):
        tiles = level_tiles[level]
        last = level == levels - 1
        setup(tiles, level > 0, last)

        def step(n, c, tiles=tiles, level=level, last=last):
            section(tiles, n, level > 0, last)
            return c

        lax.fori_loop(0, STEPS, step, 0)
        emit(tiles, level)
        if not last:
            correct(tiles)

    for level in range(levels):
        for s in range(2):
            mine = (lev == level) & (side == s)

            @pl.when(mine)
            def _(level=level, s=s):
                pltpu.make_async_copy(pack.at[level, s], recv.at[block], loc_sem.at[1]).wait()

            @pl.when(jnp.logical_not(mine))
            def _(level=level, s=s):
                out_copy(level, s).wait_send()
    for b in range(2 * levels):
        @pl.when(block != b)
        def _(b=b):
            pltpu.make_async_remote_copy(
                src_ref=pack.at[0, 0], dst_ref=recv.at[b],
                send_sem=o_send.at[0, 0], recv_sem=o_recv.at[b],
                device_id=(lev, 2 * pair + 1 - side), device_id_type=MESH,
            ).wait_recv()
    low1 = lax.broadcasted_iota(jnp.int32, (rows, LANES), 1) < HALF
    for b in range(2 * levels):
        before = (b + 2 * levels - 1) % (2 * levels)
        for q in range(2):
            for j in range(block_tiles):
                val = recv[b, j, q]
                if j == 0:
                    val = jnp.where(low1, recv[before, 0, q], val)
                at = (b * block_tiles + j) * LANES
                out_ref[0, q, :, at : at + LANES] = val


def body(u_init, v_init, feed_rate, kill_rate):
    rows, width = u_init.shape
    levels = lax.axis_size("level")
    spaces = lax.axis_size("space")
    block_tiles = width // LANES // (2 * levels)
    win = block_tiles + 1
    wide = win * LANES
    tall = 4 * rows + 2 * FAR
    needs = [
        STEPS * SWEEPS + (levels - 1 - k) * (SWEEPS * (STEPS - 1) + 1) for k in range(levels)
    ]
    level_tiles = [-(-(2 * rows + 2 * need) // SUB) for need in needs]
    tiles = level_tiles[0]
    assert tiles * SUB <= tall and needs[0] <= HALF
    f32 = jnp.float32
    ghost = (2, tiles + 2, SUB, wide)
    plain = (2, tiles, SUB, wide)
    scratch = [
        pltpu.VMEM((width // LANES + 1, 4, rows, LANES), f32),
        pltpu.VMEM((win, 4, tall, LANES), f32),
        pltpu.VMEM(plain[1:], f32),
        pltpu.VMEM(plain[1:], f32),
        pltpu.VMEM((STEPS + 1,) + ghost, f32),
        pltpu.VMEM((STEPS + 1,) + plain, f32),
        pltpu.VMEM((STEPS + 1,) + plain, f32),
        pltpu.VMEM((STEPS,) + plain, f32),
        pltpu.VMEM(ghost, f32),
        pltpu.VMEM(ghost, f32),
        pltpu.VMEM(ghost, f32),
        pltpu.VMEM((win, 2, tall, LANES), f32),
        pltpu.VMEM((STEPS, 2, win, tall, LANES), f32),
        pltpu.VMEM((levels, 2, block_tiles, 2, rows, LANES), f32),
        pltpu.VMEM((2 * levels, block_tiles, 2, rows, LANES), f32),
        pltpu.SemaphoreType.DMA((5,)),
        pltpu.SemaphoreType.DMA((5,)),
        pltpu.SemaphoreType.DMA((levels, 2)),
        pltpu.SemaphoreType.DMA((2 * levels,)),
        pltpu.SemaphoreType.DMA((2,)),
    ]
    return pl.pallas_call(
        functools.partial(kernel, levels, spaces, level_tiles, tall),
        out_shape=jax.ShapeDtypeStruct((1, 2, rows, width), f32),
        in_specs=[pl.BlockSpec(memory_space=pltpu.VMEM)] * 4,
        out_specs=pl.BlockSpec(memory_space=pltpu.VMEM),
        scratch_shapes=scratch,
        compiler_params=pltpu.CompilerParams(
            collective_id=0, has_side_effects=True, vmem_limit_bytes=56 * 1024 * 1024
        ),
    )(u_init, v_init, feed_rate, kill_rate)


def solution(mesh):
    return jax.shard_map(
        body,
        mesh=mesh,
        in_specs=(P("space", None),) * 4,
        out_specs=P("level", None, "space", None),
        check_vma=False,
    )
```

```python
import functools

import jax
import jax.numpy as jnp
from jax import lax
from jax.experimental import pallas as pl
from jax.experimental.pallas import tpu as pltpu
from jax.sharding import PartitionSpec as P

STEPS = 4
SWEEPS = 3
LANES = 128
SUB = 8
HALF = LANES // 2
FAR = 12
CHUNK = 3

DIFF = (1.0, 0.5)
INV = tuple(1.0 / (1.0 + 4.0 * d) for d in DIFF)
GAIN = tuple(d / (1.0 + 4.0 * d) for d in DIFF)
W = [
    [9.0, 19.0, -5.0, 1.0, 0.0],
    [-1.0, 13.0, 13.0, -1.0, 0.0],
    [1.0, -5.0, 19.0, 9.0, 0.0],
    [0.0, 1.0, -5.0, 19.0, 9.0],
]
MESH = pl.DeviceIdType.MESH


def kernel(
    levels, spaces, level_tiles, tall, u_ref, v_ref, f_ref, k_ref, out_ref,
    send, grid_in, feed, drain, y, lap, rea, corr, rhs, za, zb, nat, cnat, pack, recv,
    g_send, g_recv, o_send, o_recv, loc_sem,
):
    lev = lax.axis_index("level")
    spc = lax.axis_index("space")
    rows, width = u_ref.shape
    all_tiles = width // LANES
    pairs = spaces // 2
    pair, side = spc // 2, lax.rem(spc, 2)
    block_tiles = all_tiles // (2 * levels)
    win = block_tiles + 1
    nxt = lax.rem(pair + 1, pairs)
    prv = lax.rem(pair + pairs - 1, pairs)
    block = 2 * lev + side
    own_lo = FAR + rows

    for q, ref in enumerate((u_ref, v_ref, f_ref, k_ref)):
        for j in range(all_tiles + 1):
            jj = j % all_tiles
            send[j, q] = ref[:, jj * LANES : (jj + 1) * LANES]

    barrier = pltpu.get_barrier_semaphore()
    count = 0
    for p in (nxt, prv):
        for s in range(2):
            pl.semaphore_signal(barrier, inc=1, device_id=(lev, 2 * p + s), device_id_type=MESH)
            count += 1
    for dl in range(levels):
        for ds in range(2):
            if dl == 0 and ds == 0:
                continue
            pl.semaphore_signal(
                barrier, inc=1,
                device_id=(lax.rem(lev + dl, levels), 2 * pair + lax.rem(side + ds, 2)),
                device_id_type=MESH,
            )
            count += 1
    pl.semaphore_wait(barrier, count)

    def remote(win_side, r0, n, d0, sem, target, slot):
        return pltpu.make_async_remote_copy(
            src_ref=send.at[pl.ds(block_tiles * (2 * lev + win_side), win), :, pl.ds(r0, n), :],
            dst_ref=grid_in.at[:, :, pl.ds(d0, n), :],
            send_sem=g_send.at[slot], recv_sem=g_recv.at[sem],
            device_id=(lev, target), device_id_type=MESH,
        )

    def gather_copies(s):
        copies = [remote(1 - s, 0, rows, own_lo + rows * s, 0, 2 * pair + 1 - s, 0)]
        for i, t in enumerate((s, 1 - s)):
            if s == 0:
                copies.append(remote(t, rows - FAR, FAR, 0, 1, 2 * nxt + t, 1 + i))
                copies.append(remote(t, 0, rows, own_lo + 2 * rows, 3, 2 * prv + t, 3 + i))
            else:
                copies.append(remote(t, 0, rows, FAR, 2, 2 * nxt + t, 1 + i))
                copies.append(remote(t, 0, FAR, own_lo + 3 * rows, 4, 2 * prv + t, 3 + i))
        return copies

    for s in range(2):
        @pl.when(side == s)
        def _(s=s):
            for c in gather_copies(s):
                c.start()
    own = pltpu.make_async_copy(
        send.at[pl.ds(block_tiles * block, win)],
        grid_in.at[:, :, pl.ds(pl.multiple_of(own_lo + rows * side, 4), rows), :],
        loc_sem.at[0],
    )
    own.start()
    own.wait()
    for sem, n, d0 in (
        (1, FAR, 0), (2, rows, FAR), (3, rows, own_lo + 2 * rows), (4, FAR, own_lo + 3 * rows)
    ):
        remote(0, 0, n, d0, sem, 2 * nxt, 0).wait_recv()
    remote(0, 0, rows, pl.multiple_of(own_lo + rows * (1 - side), 4), 0, 2 * nxt, 0).wait_recv()
    for s in range(2):
        @pl.when(side == s)
        def _(s=s):
            for c in gather_copies(s):
                c.wait_send()

    wide = win * LANES

    def put(tiles, ref, q, a, b, val):
        ref[q, a + 1 : b + 1] = val
        if a == 0:
            ref[q, tiles + 1] = pltpu.roll(val[0], SUB - 1, 0)
        if b == tiles:
            ref[q, 0] = pltpu.roll(val[b - a - 1], 1, 0)

    def around(ref, q, a, b):
        mid = ref[q, a + 1 : b + 1]
        flat = mid.reshape((b - a) * SUB, wide)
        cols = pltpu.roll(flat, 1, 1) + pltpu.roll(flat, wide - 1, 1)
        return (ref[q, a:b] + ref[q, a + 2 : b + 2]) + cols.reshape(b - a, SUB, wide), mid

    def rates(tiles, node, last=False):
        for a, b in chunks_of(tiles):
            nu, u = around(y.at[node], 0, a, b)
            nv, v = around(y.at[node], 1, a, b)
            if not last:
                lap[node, 0, a:b] = DIFF[0] * (nu - 4.0 * u)
                lap[node, 1, a:b] = DIFF[1] * (nv - 4.0 * v)
            uvv = u * v * v
            rea[node, 0, a:b] = feed[a:b] * (1.0 - u) - uvv
            rea[node, 1, a:b] = uvv - drain[a:b] * v

    def setup(tiles, corrected, last):
        start = (tall - tiles * SUB) // 2
        for t in range(tiles):
            def window(ref, t=t):
                return jnp.concatenate(
                    [ref(j)[pl.ds(start + t, SUB, stride=tiles), :] for j in range(win)], axis=1
                )
            fd = window(lambda j: grid_in.at[j, 2])
            feed[t] = fd
            drain[t] = fd + window(lambda j: grid_in.at[j, 3])
            for q in range(2):
                put(tiles, y.at[0], q, t, t + 1, window(lambda j, q=q: grid_in.at[j, q])[None])
                if corrected:
                    for n in range(STEPS):
                        corr[n, q, t] = window(lambda j, q=q, n=n: cnat.at[n, q, j])
        rates(tiles, 0, last)

    def chunks_of(tiles):
        return [(a, min(a + CHUNK, tiles)) for a in range(0, tiles, CHUNK)]

    def section(tiles, n, corrected, last):
        for q in range(2):
            for a, b in chunks_of(tiles):
                src = y[n, q, a + 1 : b + 1] + rea[n, q, a:b]
                if corrected:
                    src = src + corr[n, q, a:b]
                put(tiles, rhs, q, a, b, src * INV[q])
        for old, new, coef in ((rhs, za, DIFF), (za, zb, GAIN), (zb, y.at[n + 1], GAIN)):
            for q in range(2):
                for a, b in chunks_of(tiles):
                    total, _ = around(old, q, a, b)
                    put(tiles, new, q, a, b, rhs[q, a + 1 : b + 1] + coef[q] * total)
        rates(tiles, n + 1, last)

    def out_copy(level, s):
        return pltpu.make_async_remote_copy(
            src_ref=pack.at[level, s], dst_ref=recv.at[block],
            send_sem=o_send.at[level, s], recv_sem=o_recv.at[block],
            device_id=(level, 2 * pair + s), device_id_type=MESH,
        )

    low = lax.broadcasted_iota(jnp.int32, (2 * rows, LANES), 1) < HALF

    def emit(tiles, level):
        start = (tall - tiles * SUB) // 2
        for q in range(2):
            for t in range(tiles):
                row = y[STEPS, q, t + 1]
                for j in range(win):
                    nat[j, q, pl.ds(start + t, SUB, stride=tiles), :] = row[:, j * LANES : (j + 1) * LANES]
            for j in range(block_tiles):
                val = nat[j, q, own_lo : own_lo + 2 * rows]
                if j == 0:
                    val = jnp.where(low, nat[block_tiles, q, own_lo : own_lo + 2 * rows], val)
                for s in range(2):
                    pack[level, s, j, q] = val[s * rows : (s + 1) * rows]
        for s in range(2):
            mine = (level == lev) & (side == s)

            @pl.when(mine)
            def _(s=s):
                pltpu.make_async_copy(pack.at[level, s], recv.at[block], loc_sem.at[1]).start()

            @pl.when(jnp.logical_not(mine))
            def _(s=s):
                out_copy(level, s).start()

    def correct(tiles):
        start = (tall - tiles * SUB) // 2
        for t in range(tiles):
            for q in range(2):
                laps = [lap[m, q, t] for m in range(STEPS + 1)]
                reas = [rea[m, q, t] for m in range(STEPS + 1)]
                both = [a + b for a, b in zip(laps, reas)]
                for n in range(STEPS):
                    acc = -laps[n + 1] - reas[n]
                    for m in range(STEPS + 1):
                        if W[n][m] != 0.0:
                            acc = acc + (W[n][m] / 24.0) * both[m]
                    for j in range(win):
                        cnat[n, q, j, pl.ds(start + t, SUB, stride=tiles), :] = acc[
                            :, j * LANES : (j + 1) * LANES
                        ]

    for level in range(levels):
        tiles = level_tiles[level]
        last = level == levels - 1
        setup(tiles, level > 0, last)

        def step(n, c, tiles=tiles, level=level, last=last):
            section(tiles, n, level > 0, last)
            return c

        lax.fori_loop(0, STEPS, step, 0)
        emit(tiles, level)
        if not last:
            correct(tiles)

    for level in range(levels):
        for s in range(2):
            mine = (lev == level) & (side == s)

            @pl.when(mine)
            def _(level=level, s=s):
                pltpu.make_async_copy(pack.at[level, s], recv.at[block], loc_sem.at[1]).wait()

            @pl.when(jnp.logical_not(mine))
            def _(level=level, s=s):
                out_copy(level, s).wait_send()
    for b in range(2 * levels):
        @pl.when(block != b)
        def _(b=b):
            pltpu.make_async_remote_copy(
                src_ref=pack.at[0, 0], dst_ref=recv.at[b],
                send_sem=o_send.at[0, 0], recv_sem=o_recv.at[b],
                device_id=(lev, 2 * pair + 1 - side), device_id_type=MESH,
            ).wait_recv()
    low1 = lax.broadcasted_iota(jnp.int32, (rows, LANES), 1) < HALF
    for b in range(2 * levels):
        before = (b + 2 * levels - 1) % (2 * levels)
        for q in range(2):
            for j in range(block_tiles):
                val = recv[b, j, q]
                if j == 0:
                    val = jnp.where(low1, recv[before, 0, q], val)
                at = (b * block_tiles + j) * LANES
                out_ref[0, q, :, at : at + LANES] = val


def body(u_init, v_init, feed_rate, kill_rate):
    rows, width = u_init.shape
    levels = lax.axis_size("level")
    spaces = lax.axis_size("space")
    block_tiles = width // LANES // (2 * levels)
    win = block_tiles + 1
    wide = win * LANES
    tall = 4 * rows + 2 * FAR
    needs = [
        STEPS * SWEEPS + (levels - 1 - k) * (SWEEPS * (STEPS - 1) + 1) for k in range(levels)
    ]
    level_tiles = [-(-(2 * rows + 2 * need) // SUB) for need in needs]
    tiles = level_tiles[0]
    assert tiles * SUB <= tall and needs[0] <= HALF
    f32 = jnp.float32
    ghost = (2, tiles + 2, SUB, wide)
    plain = (2, tiles, SUB, wide)
    scratch = [
        pltpu.VMEM((width // LANES + 1, 4, rows, LANES), f32),
        pltpu.VMEM((win, 4, tall, LANES), f32),
        pltpu.VMEM(plain[1:], f32),
        pltpu.VMEM(plain[1:], f32),
        pltpu.VMEM((STEPS + 1,) + ghost, f32),
        pltpu.VMEM((STEPS + 1,) + plain, f32),
        pltpu.VMEM((STEPS + 1,) + plain, f32),
        pltpu.VMEM((STEPS,) + plain, f32),
        pltpu.VMEM(ghost, f32),
        pltpu.VMEM(ghost, f32),
        pltpu.VMEM(ghost, f32),
        pltpu.VMEM((win, 2, tall, LANES), f32),
        pltpu.VMEM((STEPS, 2, win, tall, LANES), f32),
        pltpu.VMEM((levels, 2, block_tiles, 2, rows, LANES), f32),
        pltpu.VMEM((2 * levels, block_tiles, 2, rows, LANES), f32),
        pltpu.SemaphoreType.DMA((5,)),
        pltpu.SemaphoreType.DMA((5,)),
        pltpu.SemaphoreType.DMA((levels, 2)),
        pltpu.SemaphoreType.DMA((2 * levels,)),
        pltpu.SemaphoreType.DMA((2,)),
    ]
    return pl.pallas_call(
        functools.partial(kernel, levels, spaces, level_tiles, tall),
        out_shape=jax.ShapeDtypeStruct((1, 2, rows, width), f32),
        in_specs=[pl.BlockSpec(memory_space=pltpu.VMEM)] * 4,
        out_specs=pl.BlockSpec(memory_space=pltpu.VMEM),
        scratch_shapes=scratch,
        compiler_params=pltpu.CompilerParams(
            collective_id=0, has_side_effects=True, vmem_limit_bytes=56 * 1024 * 1024
        ),
    )(u_init, v_init, feed_rate, kill_rate)


def solution(mesh):
    return jax.shard_map(
        body,
        mesh=mesh,
        in_specs=(P("space", None),) * 4,
        out_specs=P("level", None, "space", None),
        check_vma=False,
    )
```
